32 devices in a mesh: rep: 8 (over z, core), exp: 4 (over y, x).
Axes of the slice: x: 2, y: 2, z: 4, core: 2. Of those that a mesh axis runs over, the one named last changes fastest.
Arguments:
- latents: float32 [16, 32, 2048], P('rep', None, 'exp'), may hold values from -6 to 6
- latent_mean: float32 [16, 32, 2048], P('rep', None, 'exp'), may hold values from -0.12 to 0.12
- latent_square: float32 [16, 32, 2048], P('rep', None, 'exp'), may hold values from 0.0001 to 0.01
- weight_one: bfloat16 [16, 64, 256], P('exp'), may hold values from -0.75 to 0.75
- weight_two: bfloat16 [16, 256, 256], P('exp'), may hold values from -0.375 to 0.375
- weight_three: bfloat16 [16, 3, 256], P('exp'), may hold values from -0.375 to 0.375
- dir_table: bfloat16 [256, 32], replicated, may hold values from -6 to 6
- materials: int32 [65536, 1], P(('rep', 'exp')), may hold values from 0 to 15; in each aligned block of 2048 rows (0 to 2047, 2048 to 4095, ...) at most 256 rows name the same one
- tile_ids: int32 [65536], P(('rep', 'exp')), may hold values from 0 to 1
- texel_ids: int32 [65536], P(('rep', 'exp')), may hold values from 0 to 2047
- dir_ids: int32 [65536], P(('rep', 'exp')), may hold values from 0 to 255
- targets: float32 [3, 65536], P(None, ('rep', 'exp')), may hold values from -12 to 12
Outputs:
- new_latents: float32 [16, 32, 2048], P('rep', None, 'exp')
- new_mean: float32 [16, 32, 2048], P('rep', None, 'exp')
- new_square: float32 [16, 32, 2048], P('rep', None, 'exp')
- predictions: float32 [3, 65536], P(None, ('rep', 'exp'))
- grad_one: float32 [16, 64, 256], P('exp')
- grad_two: float32 [16, 256, 256], P('exp')
- grad_three: float32 [16, 3, 256], P('exp')
The draws below stay inside these ranges and needn't reach their ends.
Inputs may be any that keep to these rules, and one draw needn't show every extreme that they name: `materials`: within the rows of one device no material is named by more than 256 rows, a bound that some block reaches.
All inputs are finite; a program needn't handle non-finite values.
Results may differ from the reference program's by a relative error of at most 0.02.
Values may be sent and summed in bfloat16 or wider, within the bound.
A program may use at most 64 MiB of HBM per device.

```python
import math
import jax
import jax.numpy as jnp
import numpy as np
from jax import lax

LAT = 32
DIRF = 32
HID = 256
OUTC = 3
NDIR = 256
TILE_DEV = 2
TEXELS = 2048
S_DEV = 2048
EXPERTS = 16
CAP = 256
SAMPLES = 65536
TILES = 16
N_REP = 8
N_EXP = 4


def set_ends(values, key, low, top_value):
    extent = values.shape
    index_at = [jax.random.randint(jax.random.fold_in(key, axis), (), 0, extent[axis]) for axis in range(len(extent))]
    values = values.at[tuple(index_at)].set(low)
    longest = extent.index(max(extent))
    index_at[longest] = (index_at[longest] + 1) % extent[longest]
    return values.at[tuple(index_at)].set(top_value)


def block_levels(own_key, shape, cuts, smallest, top_value):
    gain, own = 1.0, jax.random.fold_in(own_key, 6)
    for dim, blocks in cuts:
        steps = jnp.exp(jax.random.uniform(jax.random.fold_in(own, dim), (blocks,), jnp.float32, smallest / len(cuts), top_value / len(cuts)))
        gain = gain * jnp.repeat(steps, shape[dim] // blocks).reshape([-1 if axis == dim else 1 for axis in range(len(shape))])
    return gain


def routed_block(key, own, number, rows, count, top, bound, slope):
    sequence = jax.random.permutation(key, count)
    packed, common = shares(count, rows * top, bound, slope, True), shares(count, rows * top, bound, slope, False)
    places = jnp.arange(count)

    def named(tallies, rotation):
        used = int((tallies > 0).sum())
        fixed = max(1, used // 4)
        moved = fixed + (places - fixed + rotation * (used - fixed)) % max(1, count - fixed)
        return jnp.zeros((count,), jnp.int32).at[sequence[jnp.where(places < fixed, places, moved)]].set(jnp.asarray(tallies, jnp.int32))

    tallies = jnp.where(number % 4 == 0, named(packed, number // 4), named(common, number - number // 4 - 1))
    mixed = jax.random.permutation(jax.random.fold_in(own, 3), count)
    source_of, receiver = mixed[0:count // 2 * 2:2], mixed[1:count // 2 * 2:2]
    room = jnp.minimum(tallies[source_of] - 1, bound - tallies[receiver]) // 2
    room = jnp.where((source_of == sequence[0]) | (receiver == sequence[0]) | (tallies[receiver] == 0), 0, jnp.maximum(room, 0))
    moved = jax.random.randint(jax.random.fold_in(own, 4), (count // 2,), 0, 1 << 20) % (room + 1)
    tallies = tallies.at[source_of].add(-moved).at[receiver].add(moved)
    items = jnp.searchsorted(jnp.cumsum(tallies), jnp.arange(rows * top), side="right").astype(jnp.int32)
    listing = items.reshape(top, rows).T
    listing = listing[jax.random.permutation(jax.random.fold_in(own, 1), rows)]
    rotation = jax.random.randint(jax.random.fold_in(own, 2), (rows, 1), 0, top)
    return jnp.take_along_axis(listing, (jnp.arange(top)[None, :] + rotation) % top, axis=1)


def shares(number_of, total, bound, lean, full):
    weights = [(1 << 20) // math.isqrt(rank ** lean) + 1 for rank in range(1, number_of + 1)]
    largest = bound if full else min(bound, max(-(-total // number_of), total * weights[0] // sum(weights)))
    least = 1 if total - largest >= number_of - 1 else 0
    counts, rest = [largest] + [least] * (number_of - 1), total - largest - least * (number_of - 1)
    while rest > 0:
        candidates = [i for i in range(1, number_of) if counts[i] < largest] or [i for i in range(1, number_of) if counts[i] < bound]
        whole, budget = sum([weights[i] for i in candidates]), rest
        for i in candidates:
            more = min(bound - counts[i], max(1, budget * weights[i] // whole), rest)
            counts[i] = counts[i] + more
            rest = rest - more
    return np.array(counts)


def normal_values(key, extent, deviation, bound, pieces=(), kind=jnp.bfloat16):
    array = jax.random.normal(key, extent, jnp.float32) * deviation
    if len(pieces) > 0:
        array = block_levels(key, extent, pieces, -0.22, 0.18) * array
    return jnp.clip(array, min=-bound, max=bound).astype(kind)


def setup_inputs(seed: int = 0) -> dict:
    keys = jax.random.split(jax.random.key(seed), 13)
    latents = normal_values(keys[0], (TILES, LAT, TEXELS), 1.0, 6.0, ((0, 8), (2, 4)), jnp.float32)
    latent_mean = normal_values(keys[1], (TILES, LAT, TEXELS), 0.02, 0.12, ((0, 8), (2, 4)), jnp.float32)
    latent_square = jnp.clip(jnp.exp(math.log(0.01) - 4.6051702 * jax.random.uniform(keys[2], (TILES, LAT, TEXELS), jnp.float32) ** block_levels(keys[2], (TILES, LAT, TEXELS), ((0, 8), (2, 4)), -0.2, 0.2)), 0.0001, 0.01)
    weight_one = normal_values(keys[3], (EXPERTS, LAT + DIRF, HID), (LAT + DIRF) ** -0.5, 0.75, ((0, 4),))
    weight_two = normal_values(keys[4], (EXPERTS, HID, HID), HID ** -0.5, 0.375, ((0, 4),))
    weight_three = normal_values(keys[5], (EXPERTS, OUTC, HID), HID ** -0.5, 0.375, ((0, 4),))
    dir_table = normal_values(keys[6], (NDIR, DIRF), 1.0, 6.0)
    materials_keys = jax.random.split(jax.random.fold_in(keys[7], 1), SAMPLES // S_DEV)
    materials_turns = jax.random.permutation(jax.random.fold_in(keys[7], 3), SAMPLES // S_DEV)
    materials = jax.vmap(lambda own, number: routed_block(jax.random.fold_in(keys[7], 2), own, number, S_DEV, EXPERTS, 1, CAP, 2))(materials_keys, materials_turns).reshape((SAMPLES, 1))
    tile_ids = set_ends(jax.random.randint(keys[8], (SAMPLES,), 0, TILE_DEV), jax.random.fold_in(keys[8], 1), 0, TILE_DEV - 1).astype(jnp.int32)
    texel_ids = set_ends(jax.random.randint(keys[9], (SAMPLES,), 0, TEXELS), jax.random.fold_in(keys[9], 1), 0, TEXELS - 1).astype(jnp.int32)
    dir_ids = set_ends(jax.random.randint(keys[10], (SAMPLES,), 0, NDIR), jax.random.fold_in(keys[10], 1), 0, NDIR - 1).astype(jnp.int32)
    targets = normal_values(keys[11], (OUTC, SAMPLES), 2.0, 12.0, ((1, 32),), jnp.float32)
    return dict(latents=latents, latent_mean=latent_mean, latent_square=latent_square, weight_one=weight_one, weight_two=weight_two, weight_three=weight_three, dir_table=dir_table, materials=materials, tile_ids=tile_ids, texel_ids=texel_ids, dir_ids=dir_ids, targets=targets)


decay_one = 0.9
decay_two = 0.99
step_rate = 0.05
epsilon = 1e-08

def silu_slope(preact):
    sigmoid_v = jax.nn.sigmoid(preact)
    return sigmoid_v * (1.0 + preact * (1.0 - sigmoid_v))

def expert_step(inputs, target_rows, layer_one, layer_two, layer_three):
    pre_one = jnp.dot(inputs, layer_one, preferred_element_type=jnp.float32)
    act_one = jax.nn.silu(pre_one).astype(jnp.bfloat16)
    pre_two = jnp.dot(act_one, layer_two, preferred_element_type=jnp.float32)
    act_two = jax.nn.silu(pre_two).astype(jnp.bfloat16)
    predicted = lax.dot_general(act_two, layer_three, (((1,), (1,)), ((), ())), preferred_element_type=jnp.float32)
    misfit = (predicted - target_rows).astype(jnp.bfloat16)
    grad_three = lax.dot_general(misfit, act_two, (((0,), (0,)), ((), ())), preferred_element_type=jnp.float32)
    back_two = jnp.dot(misfit, layer_three, preferred_element_type=jnp.float32)
    delta_two = (back_two * silu_slope(pre_two)).astype(jnp.bfloat16)
    grad_two = lax.dot_general(act_one, delta_two, (((0,), (0,)), ((), ())), preferred_element_type=jnp.float32)
    back_one = lax.dot_general(delta_two, layer_two, (((1,), (1,)), ((), ())), preferred_element_type=jnp.float32)
    delta_one = (back_one * silu_slope(pre_one)).astype(jnp.bfloat16)
    grad_one = lax.dot_general(inputs, delta_one, (((0,), (0,)), ((), ())), preferred_element_type=jnp.float32)
    latent_part = layer_one[:LAT]
    latent_rows = lax.dot_general(delta_one, latent_part, (((1,), (1,)), ((), ())), preferred_element_type=jnp.float32)
    return (latent_rows.astype(jnp.bfloat16), predicted, grad_one, grad_two, grad_three)

def reference(latents, latent_mean, latent_square, weight_one, weight_two, weight_three, dir_table, materials, tile_ids, texel_ids, dir_ids, targets):
    devices = N_REP * N_EXP
    samples = materials.shape[0]
    material = materials[:, 0]
    one_hot = (material[:, None] == jnp.arange(EXPERTS, dtype=jnp.int32)[None, :]).astype(jnp.int32)
    counted = jnp.cumsum(one_hot.reshape(devices, S_DEV, EXPERTS), axis=1).reshape(samples, EXPERTS)
    position = lax.optimization_barrier(jnp.sum((counted - 1) * one_hot, axis=1)).astype(jnp.int32)
    device_block = (jnp.arange(samples, dtype=jnp.int32) // S_DEV).astype(jnp.int32)
    slot_index = (device_block * CAP + position).astype(jnp.int32)
    rep_group = (device_block // N_EXP).astype(jnp.int32)
    tile_global = (rep_group * TILE_DEV + tile_ids).astype(jnp.int32)
    latent_bf = latents.astype(jnp.bfloat16)
    sample_latent = latent_bf[tile_global, :, texel_ids]
    feature_rows = jnp.concatenate([sample_latent, dir_table[dir_ids]], axis=1)
    target_cols = targets.T
    total_slots = devices * CAP

    def per_expert(expert):
        target_slot = jnp.where(material == expert, slot_index, total_slots).astype(jnp.int32)
        inputs = jnp.zeros((total_slots, feature_rows.shape[1]), jnp.bfloat16).at[target_slot].set(feature_rows, mode='drop')
        wanted = jnp.zeros((total_slots, OUTC), jnp.float32).at[target_slot].set(target_cols, mode='drop')
        return expert_step(inputs, wanted, weight_one[expert], weight_two[expert], weight_three[expert])
    latent_rows, predicted, grad_one, grad_two, grad_three = lax.map(per_expert, jnp.arange(EXPERTS, dtype=jnp.int32))
    sample_grad = latent_rows[material, slot_index].astype(jnp.float32)
    sample_pred = predicted[material, slot_index]
    texel_grad = jnp.zeros(latents.shape, jnp.float32).at[tile_global, :, texel_ids].add(sample_grad)
    new_mean = decay_one * latent_mean + (1.0 - decay_one) * texel_grad
    new_square = decay_two * latent_square + (1.0 - decay_two) * texel_grad * texel_grad
    new_latents = latents - step_rate * new_mean / (jnp.sqrt(new_square) + epsilon)
    return (new_latents, new_mean, new_square, sample_pred.T, grad_one, grad_two, grad_three)
```

```python
import functools

import jax
import jax.numpy as jnp
from jax import lax
from jax.experimental import pallas as pl
from jax.experimental.pallas import tpu as pltpu
from jax.sharding import PartitionSpec as P

BF = jnp.bfloat16
F32 = jnp.float32
MESH = pl.DeviceIdType.MESH
decay_one = 0.9
decay_two = 0.99
step_rate = 0.05
epsilon = 1e-08
VROWS = 16


def nn(a, b):
    return lax.dot_general(a, b, (((1,), (0,)), ((), ())), preferred_element_type=F32)


def nt(a, b):
    return lax.dot_general(a, b, (((1,), (1,)), ((), ())), preferred_element_type=F32)


def tn(a, b):
    return lax.dot_general(a, b, (((0,), (0,)), ((), ())), preferred_element_type=F32)


def hot(cond):
    return jnp.where(cond, 1.0, 0.0).astype(BF)


def step_kernel(
    cfg,
    lat_ref,
    mean_ref,
    sq_ref,
    w1_ref,
    w2_ref,
    w3_ref,
    dirt_ref,
    mat_ref,
    tile_ref,
    texel_ref,
    dir_ref,
    tgt_ref,
    nlat_ref,
    nmean_ref,
    nsq_ref,
    pred_ref,
    g1_ref,
    g2_ref,
    g3_ref,
    tex,
    slot_send,
    slot_recv,
    q_ref,
    ps_send,
    ps_recv,
    dg_acc,
    dg_send,
    dg_recv,
    g1_acc,
    gfull,
    hs_send,
    hs_recv,
    zs_send,
    zr_recv,
    fin,
    tex_sems,
    slot_sems,
    ps_sems,
    dg_sems,
    hs_sems,
    zr_sems,
    ag_sems,
    fw_sems,
):
    N, R, E, L = cfg["N"], cfg["R"], cfg["E"], cfg["L"]
    S, CAP, HI, LOL, LO = cfg["S"], cfg["CAP"], cfg["HI"], cfg["LOL"], cfg["LO"]
    LAT, DIRF, HID, T, Z = cfg["LAT"], cfg["DIRF"], cfg["HID"], cfg["T"], cfg["Z"]
    OUTC, CH, RC, SB = cfg["OUTC"], cfg["CH"], cfg["RC"], cfg["SB"]
    NDIR = dirt_ref.shape[0]
    PL = LOL * LAT
    K = LO * LAT
    me = lax.axis_index("exp")
    rep = lax.axis_index("rep")
    core = rep % 2
    zi = rep // 2
    mate = zi * 2 + (1 - core)

    def remote(src, dst, sems, index, peer):
        return pltpu.make_async_remote_copy(
            src_ref=src,
            dst_ref=dst,
            send_sem=sems.at[(0,) + index],
            recv_sem=sems.at[(1,) + index],
            device_id=peer,
            device_id_type=MESH,
        )

    barrier = pltpu.get_barrier_semaphore()
    for k in range(1, N):
        pl.semaphore_signal(
            barrier, inc=1, device_id={"exp": (me + k) % N}, device_id_type=MESH
        )
    pl.semaphore_signal(barrier, inc=1, device_id={"rep": mate}, device_id_type=MESH)
    for k in range(1, Z):
        pl.semaphore_signal(
            barrier,
            inc=1,
            device_id={"rep": ((zi + k) % Z) * 2 + core},
            device_id_type=MESH,
        )
    for t in range(T):
        for l in range(LOL):
            tex[me, t, l * LAT : (l + 1) * LAT, :] = lat_ref[
                t, :, l * HI : (l + 1) * HI
            ].astype(BF)
    pl.semaphore_wait(barrier, (N - 1) + 1 + (Z - 1))

    def tex_copy(k):
        return remote(tex.at[me], tex.at[me], tex_sems, (k - 1,), {"exp": (me + k) % N})

    for k in range(1, N):
        tex_copy(k).start()

    mat = mat_ref[...]
    one_hot = jnp.where(
        lax.broadcasted_iota(jnp.int32, (E, S), 0) == mat, 1.0, 0.0
    )
    W = min(256, S)
    blocks = [one_hot[:, b * W : (b + 1) * W] for b in range(S // W)]
    upper = hot(
        lax.broadcasted_iota(jnp.int32, (W, W), 0)
        <= lax.broadcasted_iota(jnp.int32, (W, W), 1)
    )
    cum = nn(jnp.concatenate(blocks, axis=0).astype(BF), upper)
    before = jnp.zeros((E, 1), F32)
    places = []
    for b in range(S // W):
        part = cum[b * E : (b + 1) * E]
        places.append(
            jnp.sum(blocks[b] * (part + (before - 1.0)), axis=0, keepdims=True)
        )
        before = before + part[:, W - 1 : W]
    position = jnp.concatenate(places, axis=1).astype(jnp.int32)
    q = hot(lax.broadcasted_iota(jnp.int32, (CAP, S), 0) == position)
    q_ref[...] = q
    tgt = tgt_ref[...]
    tgt_hi = tgt.astype(BF).astype(F32)
    tgt_lo = tgt - tgt_hi
    texel = texel_ref[...]
    values = jnp.concatenate(
        [
            tgt_hi,
            tgt_lo,
            (texel % HI + 1).astype(F32),
            (tile_ref[...] * LO + texel // HI).astype(F32),
            (dir_ref[...] + 1).astype(F32),
            jnp.zeros((VROWS - 2 * OUTC - 3, S), F32),
        ],
        axis=0,
    )
    spread = jnp.concatenate(
        [jnp.where(mat == e, values, 0.0).astype(BF) for e in range(E)], axis=0
    )
    routed = nt(spread, q).astype(BF)
    for d in range(N):
        slot_send[d] = routed[d * L * VROWS : (d + 1) * L * VROWS]

    def slot_copy(k):
        peer = (me + k) % N
        return remote(
            slot_send.at[peer], slot_recv.at[me], slot_sems, (k - 1,), {"exp": peer}
        )

    for k in range(1, N):
        slot_copy(k).start()
    slot_recv[me] = slot_send[me]
    dg_acc[...] = jnp.zeros(dg_acc.shape, F32)
    for k in range(1, N):
        tex_copy(k).wait()
    for k in range(1, N):
        slot_copy(k).wait()

    def half_copy(e):
        return remote(hs_send.at[e], hs_recv.at[e], hs_sems, (e,), {"rep": mate})

    def expert(e, carry):
        layer_one = w1_ref[e]
        layer_two = w2_ref[e]
        layer_three = jnp.concatenate(
            [w3_ref[e], jnp.zeros((VROWS - OUTC, HID), BF)], axis=0
        )
        lat_part = jnp.concatenate([layer_one[:LAT]] * LO, axis=0)
        wide_one = jnp.concatenate([lat_part, layer_one[LAT:]], axis=0)

        def chunk(b, carry):
            width = SB * CAP
            v = jnp.concatenate(
                [
                    slot_recv[b * SB + i, pl.ds(pl.multiple_of(e * VROWS, VROWS), VROWS), :]
                    for i in range(SB)
                ],
                axis=1,
            ).astype(F32)
            target = v[:OUTC] + v[OUTC : 2 * OUTC]
            hi = v[2 * OUTC : 2 * OUTC + 1]
            tlo = v[2 * OUTC + 1 : 2 * OUTC + 2]
            di = v[2 * OUTC + 2 : 2 * OUTC + 3].astype(jnp.int32)
            hi = hi.astype(jnp.int32)
            tlo = tlo.astype(jnp.int32)
            tile = tlo // LO
            low = tlo % LO
            count = lax.broadcasted_iota(jnp.int32, (HI, width), 0) + 1
            hots = [hot(count == jnp.where(tile == t, hi, 0)) for t in range(T)]
            found = jnp.zeros((K, width), F32)
            for t in range(T):
                found += nn(tex[:, t].reshape(K, HI), hots[t])
            in_low = lax.broadcasted_iota(jnp.int32, (K, width), 0) // LAT == low
            found = jnp.where(in_low, found, 0.0).astype(BF)
            dir_hot = hot(lax.broadcasted_iota(jnp.int32, (NDIR, width), 0) + 1 == di)
            dir_part = tn(dirt_ref[...], dir_hot).astype(BF)
            x = jnp.concatenate([found, dir_part], axis=0)
            pre_one = tn(wide_one, x)
            sig_one = 0.5 * jnp.tanh(0.5 * pre_one) + 0.5
            act_one = (pre_one * sig_one).astype(BF)
            slope_one = sig_one * (1.0 + pre_one * (1.0 - sig_one))
            pre_two = tn(layer_two, act_one)
            sig_two = 0.5 * jnp.tanh(0.5 * pre_two) + 0.5
            act_two = (pre_two * sig_two).astype(BF)
            slope_two = sig_two * (1.0 + pre_two * (1.0 - sig_two))
            predicted = nn(layer_three, act_two)
            for i in range(SB):
                ps_send[b * SB + i, e] = predicted[:8, i * CAP : (i + 1) * CAP]
            misfit = (
                predicted
                - jnp.concatenate([target, jnp.zeros((VROWS - OUTC, width), F32)], axis=0)
            ).astype(BF)
            grad_three = nt(misfit, act_two)
            delta_two = (tn(layer_three, misfit) * slope_two).astype(BF)
            grad_two = nt(act_one, delta_two)
            delta_one = (nn(layer_two, delta_two) * slope_one).astype(BF)
            grad_one = nt(x, delta_one)
            rows = nn(lat_part, delta_one)
            rows = jnp.where(in_low, rows, 0.0).astype(BF)
            for t in range(T):
                dg_acc[t] += nt(rows, hots[t])
            g1_acc[...] += grad_one
            gfull[e, 2 * LAT : 2 * LAT + HID] += grad_two
            gfull[e, 2 * LAT + HID : 2 * LAT + HID + VROWS] += grad_three
            return carry

        g1_acc[...] = jnp.zeros(g1_acc.shape, F32)
        gfull[e] = jnp.zeros((CH, HID), F32)
        lax.fori_loop(0, N // SB, chunk, 0)
        lat_grad = g1_acc[0:LAT]
        for l in range(1, LO):
            lat_grad = lat_grad + g1_acc[l * LAT : (l + 1) * LAT]
        gfull[e, 0:LAT] = lat_grad
        gfull[e, LAT : LAT + DIRF] = g1_acc[K:]
        theirs = gfull[e, pl.ds(pl.multiple_of((1 - core) * (CH // 2), 8), CH // 2), :]
        hs_send[e] = theirs.astype(BF)
        half_copy(e).start()
        return carry

    lax.fori_loop(0, L, expert, 0)

    def pred_copy(k):
        peer = (me + k) % N
        return remote(ps_send.at[peer], ps_recv.at[me], ps_sems, (k - 1,), {"exp": peer})

    def dense_copy(k):
        peer = (me + k) % N
        return remote(dg_send.at[peer], dg_recv.at[me], dg_sems, (k - 1,), {"exp": peer})

    for k in range(1, N):
        pred_copy(k).start()
    ps_recv[me] = ps_send[me]
    for d in range(N):
        for t in range(T):
            dg_send[d, t] = dg_acc[t, d * PL : (d + 1) * PL].astype(BF)
    for k in range(1, N):
        dense_copy(k).start()

    def z_copy(k):
        there = (zi + k) % Z
        return remote(
            zs_send.at[there], zr_recv.at[zi], zr_sems, (k - 1,), {"rep": there * 2 + core}
        )

    def gather_copy(k):
        there = (zi + k) % Z
        return remote(
            fin.at[core, zi], fin.at[core, zi], ag_sems, (k - 1,), {"rep": there * 2 + core}
        )

    def forward_copy(k):
        owner = (zi + Z - k) % Z
        return remote(
            fin.at[core, owner], fin.at[core, owner], fw_sems, (k,), {"rep": mate}
        )

    for e in range(L):
        half_copy(e).wait()
        for z in range(Z):
            own = gfull[e, pl.ds(pl.multiple_of(core * (CH // 2) + z * RC, 8), RC), :]
            zs_send[z, e] = (own + hs_recv[e, z * RC : (z + 1) * RC].astype(F32)).astype(BF)
    for k in range(1, Z):
        z_copy(k).start()

    for k in range(1, N):
        dense_copy(k).wait()
    for t in range(T):
        grad = dg_acc[t, pl.ds(pl.multiple_of(me * PL, 8), PL), :]
        for k in range(1, N):
            grad = grad + dg_recv[(me + k) % N, t].astype(F32)
        for l in range(LOL):
            lanes = slice(l * HI, (l + 1) * HI)
            g = grad[l * LAT : (l + 1) * LAT]
            new_mean = decay_one * mean_ref[t, :, lanes] + (1.0 - decay_one) * g
            new_sq = decay_two * sq_ref[t, :, lanes] + (1.0 - decay_two) * g * g
            nmean_ref[t, :, lanes] = new_mean
            nsq_ref[t, :, lanes] = new_sq
            nlat_ref[t, :, lanes] = lat_ref[t, :, lanes] - step_rate * new_mean / (
                jnp.sqrt(new_sq) + epsilon
            )

    for k in range(1, Z):
        z_copy(k).wait()
    total = zs_send[zi].astype(F32)
    for k in range(1, Z):
        total = total + zr_recv[(zi + k) % Z].astype(F32)
    fin[core, zi] = total.astype(BF)
    for k in range(1, Z):
        gather_copy(k).start()
    forward_copy(0).start()

    for k in range(1, N):
        pred_copy(k).wait()
    slots = ps_recv[...].reshape(E * 8, CAP)
    slots_hi = slots.astype(BF)
    slots_lo = (slots - slots_hi.astype(F32)).astype(BF)
    back = nn(slots_hi, q_ref[...]) + nn(slots_lo, q_ref[...])
    mat = mat_ref[...]
    mine = jnp.zeros((8, S), F32)
    for e in range(E):
        mine = mine + jnp.where(mat == e, back[e * 8 : (e + 1) * 8], 0.0)
    pred_ref[...] = mine[:OUTC]

    for k in range(1, Z):
        gather_copy(k).wait()
        forward_copy(k).start()
    for k in range(Z):
        forward_copy(k).wait()
    for e in range(L):
        for h in range(2):
            for z in range(Z):
                start = (h * Z + z) * RC
                gfull[e, start : start + RC] = fin[h, z, e].astype(F32)
        g1_ref[e] = gfull[e, 0 : LAT + DIRF]
        g2_ref[e] = gfull[e, LAT + DIRF : LAT + DIRF + HID]
        g3_ref[e] = gfull[e, LAT + DIRF + HID : LAT + DIRF + HID + OUTC]


def on_device(N, R, *args):
    latents, _, _, weight_one, weight_two, weight_three, dir_table = args[:7]
    materials, tile_ids, texel_ids, dir_ids, targets = args[7:]
    T, LAT, texl = latents.shape
    L, width, HID = weight_one.shape
    OUTC = weight_three.shape[1]
    DIRF = dir_table.shape[1]
    S = materials.shape[0]
    E = L * N
    CAP = max(128, 2 * S // E)
    HI = min(256, texl)
    LOL = texl // HI
    LO = N * LOL
    Z = R // 2
    unit = 8 * R
    CH = -(-(width + HID + VROWS) // unit) * unit
    RC = CH // R
    K = LO * LAT
    cfg = dict(
        N=N, R=R, E=E, L=L, S=S, CAP=CAP, HI=HI, LOL=LOL, LO=LO, LAT=LAT, DIRF=DIRF,
        HID=HID, T=T, Z=Z, OUTC=OUTC, CH=CH, RC=RC, SB=2,
    )
    flat = [a.reshape(1, S) for a in (materials, tile_ids, texel_ids, dir_ids)]
    vmem = pl.BlockSpec(memory_space=pltpu.VMEM)
    outs = (
        jax.ShapeDtypeStruct(latents.shape, F32),
        jax.ShapeDtypeStruct(latents.shape, F32),
        jax.ShapeDtypeStruct(latents.shape, F32),
        jax.ShapeDtypeStruct(targets.shape, F32),
        jax.ShapeDtypeStruct(weight_one.shape, F32),
        jax.ShapeDtypeStruct(weight_two.shape, F32),
        jax.ShapeDtypeStruct(weight_three.shape, F32),
    )
    dma = pltpu.SemaphoreType.DMA
    scratch = [
        pltpu.VMEM((N, T, LOL * LAT, HI), BF),
        pltpu.VMEM((N, L * VROWS, CAP), BF),
        pltpu.VMEM((N, L * VROWS, CAP), BF),
        pltpu.VMEM((CAP, S), BF),
        pltpu.VMEM((N, L, 8, CAP), F32),
        pltpu.VMEM((N, L, 8, CAP), F32),
        pltpu.VMEM((T, K, HI), F32),
        pltpu.VMEM((N, T, LOL * LAT, HI), BF),
        pltpu.VMEM((N, T, LOL * LAT, HI), BF),
        pltpu.VMEM((K + DIRF, HID), F32),
        pltpu.VMEM((L, CH, HID), F32),
        pltpu.VMEM((L, CH // 2, HID), BF),
        pltpu.VMEM((L, CH // 2, HID), BF),
        pltpu.VMEM((Z, L, RC, HID), BF),
        pltpu.VMEM((Z, L, RC, HID), BF),
        pltpu.VMEM((2, Z, L, RC, HID), BF),
        dma((2, N - 1)),
        dma((2, N - 1)),
        dma((2, N - 1)),
        dma((2, N - 1)),
        dma((2, L)),
        dma((2, Z - 1)),
        dma((2, Z - 1)),
        dma((2, Z)),
    ]
    return pl.pallas_call(
        functools.partial(step_kernel, cfg),
        out_shape=outs,
        in_specs=[vmem] * 12,
        out_specs=tuple([vmem] * 7),
        scratch_shapes=scratch,
        compiler_params=pltpu.CompilerParams(
            collective_id=0, has_side_effects=True, vmem_limit_bytes=50 * 2**20
        ),
    )(*args[:7], *flat, targets)


def solution(mesh):
    tex = P("rep", None, "exp")
    own = P("exp", None, None)
    rows = P(("rep", "exp"))
    in_specs = (
        tex, tex, tex, own, own, own, P(), P(("rep", "exp"), None), rows, rows, rows,
        P(None, ("rep", "exp")),
    )
    out_specs = (tex, tex, tex, P(None, ("rep", "exp")), own, own, own)
    return jax.shard_map(
        functools.partial(on_device, mesh.shape["exp"], mesh.shape["rep"]),
        mesh=mesh,
        in_specs=in_specs,
        out_specs=out_specs,
        check_vma=False,
    )
```

```python
import functools

import jax
import jax.numpy as jnp
from jax import lax
from jax.experimental import pallas as pl
from jax.experimental.pallas import tpu as pltpu
from jax.sharding import PartitionSpec as P

BF = jnp.bfloat16
F32 = jnp.float32
MESH = pl.DeviceIdType.MESH
decay_one = 0.9
decay_two = 0.99
step_rate = 0.05
epsilon = 1e-08
VROWS = 16


def nn(a, b):
    return lax.dot_general(a, b, (((1,), (0,)), ((), ())), preferred_element_type=F32)


def nt(a, b):
    return lax.dot_general(a, b, (((1,), (1,)), ((), ())), preferred_element_type=F32)


def tn(a, b):
    return lax.dot_general(a, b, (((0,), (0,)), ((), ())), preferred_element_type=F32)


def hot(cond):
    return jnp.where(cond, 1.0, 0.0).astype(BF)


def step_kernel(
    cfg,
    *refs,
):
    hbm_in, hbm_out, rest = refs[:12], refs[12:19], refs[19:]
    (
        lat_ref,
        mean_ref,
        sq_ref,
        w1_ref,
        w2_ref,
        w3_ref,
        dirt_ref,
        mat_ref,
        tile_ref,
        texel_ref,
        dir_ref,
        tgt_ref,
    ) = rest[:12]
    (
        nlat_ref,
        nmean_ref,
        nsq_ref,
        pred_ref,
        g3_ref,
    ) = rest[12:17]
    (
        tex,
        slot_send,
        slot_recv,
        q_ref,
        ps_send,
        ps_recv,
        dg_acc,
        dg_send,
        dg_recv,
        g1_acc,
        gfull,
        hs_send,
        hs_recv,
        zs_send,
        zr_recv,
        fin,
        w3p,
        texture,
        tex_sems,
        slot_sems,
        ps_sems,
        dg_sems,
        hs_sems,
        zr_sems,
        ag_sems,
        fw_sems,
        in_sems,
        out_sems,
        grad_sems,
    ) = rest[17:]
    N, R, E, L = cfg["N"], cfg["R"], cfg["E"], cfg["L"]
    S, CAP, HI, LOL, LO = cfg["S"], cfg["CAP"], cfg["HI"], cfg["LOL"], cfg["LO"]
    LAT, DIRF, HID, T, Z = cfg["LAT"], cfg["DIRF"], cfg["HID"], cfg["T"], cfg["Z"]
    OUTC, CH, RC, SB = cfg["OUTC"], cfg["CH"], cfg["RC"], cfg["SB"]
    NDIR = dirt_ref.shape[1]
    PL = LOL * LAT
    K = LO * LAT
    first = LAT + DIRF + HID
    me = lax.axis_index("exp")
    rep = lax.axis_index("rep")
    core = rep % 2
    zi = rep // 2
    mate = zi * 2 + (1 - core)

    def remote(src, dst, sems, index, peer):
        return pltpu.make_async_remote_copy(
            src_ref=src,
            dst_ref=dst,
            send_sem=sems.at[(0,) + index],
            recv_sem=sems.at[(1,) + index],
            device_id=peer,
            device_id_type=MESH,
        )

    def load(i):
        return pltpu.make_async_copy(hbm_in[i], rest[i], in_sems.at[i])

    def save(i):
        return pltpu.make_async_copy(rest[12 + min(i, 4)], hbm_out[i], out_sems.at[i])

    barrier = pltpu.get_barrier_semaphore()
    for k in range(1, N):
        pl.semaphore_signal(
            barrier, inc=1, device_id={"exp": (me + k) % N}, device_id_type=MESH
        )
    pl.semaphore_signal(barrier, inc=1, device_id={"rep": mate}, device_id_type=MESH)
    for k in range(1, Z):
        pl.semaphore_signal(
            barrier,
            inc=1,
            device_id={"rep": ((zi + k) % Z) * 2 + core},
            device_id_type=MESH,
        )
    for i in (0, 7, 8, 9, 10, 11, 6, 3, 4, 5, 1, 2):
        load(i).start()
    load(0).wait()
    for t in range(T):
        for l in range(LOL):
            tex[me, t, l * LAT : (l + 1) * LAT, :] = lat_ref[
                t, :, l * HI : (l + 1) * HI
            ].astype(BF)
    pl.semaphore_wait(barrier, (N - 1) + 1 + (Z - 1))

    def tex_copy(k):
        return remote(tex.at[me], tex.at[me], tex_sems, (k - 1,), {"exp": (me + k) % N})

    for k in range(1, N):
        tex_copy(k).start()

    for i in range(7, 12):
        load(i).wait()
    mat = mat_ref[...]
    one_hot = jnp.where(
        lax.broadcasted_iota(jnp.int32, (E, S), 0) == mat, 1.0, 0.0
    )
    W = min(256, S)
    blocks = [one_hot[:, b * W : (b + 1) * W] for b in range(S // W)]
    upper = hot(
        lax.broadcasted_iota(jnp.int32, (W, W), 0)
        <= lax.broadcasted_iota(jnp.int32, (W, W), 1)
    )
    cum = nn(jnp.concatenate(blocks, axis=0).astype(BF), upper)
    before = jnp.zeros((E, 1), F32)
    places = []
    for b in range(S // W):
        part = cum[b * E : (b + 1) * E]
        places.append(
            jnp.sum(blocks[b] * (part + (before - 1.0)), axis=0, keepdims=True)
        )
        before = before + part[:, W - 1 : W]
    position = jnp.concatenate(places, axis=1).astype(jnp.int32)
    q = hot(lax.broadcasted_iota(jnp.int32, (CAP, S), 0) == position)
    q_ref[...] = q
    tgt = tgt_ref[...]
    tgt_hi = tgt.astype(BF).astype(F32)
    tgt_lo = tgt - tgt_hi
    texel = texel_ref[...]
    values = jnp.concatenate(
        [
            tgt_hi,
            tgt_lo,
            (texel % HI + 1).astype(F32),
            (tile_ref[...] * LO + texel // HI).astype(F32),
            (dir_ref[...] + 1).astype(F32),
            jnp.zeros((VROWS - 2 * OUTC - 3, S), F32),
        ],
        axis=0,
    )
    spread = jnp.concatenate(
        [jnp.where(mat == e, values, 0.0).astype(BF) for e in range(E)], axis=0
    )
    routed = nt(spread, q).astype(BF)
    for d in range(N):
        slot_send[d] = routed[d * L * VROWS : (d + 1) * L * VROWS]

    def slot_copy(k):
        peer = (me + k) % N
        return remote(
            slot_send.at[peer], slot_recv.at[me], slot_sems, (k - 1,), {"exp": peer}
        )

    for k in range(1, N):
        slot_copy(k).start()
    slot_recv[me] = slot_send[me]
    dg_acc[...] = jnp.zeros(dg_acc.shape, F32)
    for i in range(1, 7):
        load(i).wait()
    colour = w3_ref[...].astype(F32)
    for e in range(L):
        w3p[e] = jnp.concatenate(
            [colour[c, e : e + 1] for c in range(OUTC)]
            + [jnp.zeros((VROWS - OUTC, HID), F32)],
            axis=0,
        ).astype(BF)
    for k in range(1, N):
        tex_copy(k).wait()
    for t in range(T):
        for d in range(N):
            texture[d * PL : (d + 1) * PL, t * HI : (t + 1) * HI] = tex[d, t]
    for k in range(1, N):
        slot_copy(k).wait()

    def half_copy(e):
        return remote(hs_send.at[e], hs_recv.at[e], hs_sems, (e,), {"rep": mate})

    def z_copy(e, k):
        there = (zi + k) % Z
        return remote(
            zs_send.at[e, there],
            zr_recv.at[e, zi],
            zr_sems,
            (e, k - 1),
            {"rep": there * 2 + core},
        )

    def gather_copy(e, k):
        there = (zi + k) % Z
        piece = fin.at[e, core, zi]
        return remote(piece, piece, ag_sems, (e, k - 1), {"rep": there * 2 + core})

    def forward_copy(e, k):
        piece = fin.at[e, core, (zi + Z - k) % Z]
        return remote(piece, piece, fw_sems, (e, k), {"rep": mate})

    def halves(e):
        half_copy(e).wait()
        for z in range(Z):
            own = gfull[e, pl.ds(pl.multiple_of(core * (CH // 2) + z * RC, 8), RC), :]
            zs_send[e, z] = (own + hs_recv[e, z].astype(F32)).astype(BF)
        for k in range(1, Z):
            z_copy(e, k).start()

    def parts(e):
        for k in range(1, Z):
            z_copy(e, k).wait()
        total = zs_send[e, zi].astype(F32)
        for k in range(1, Z):
            total = total + zr_recv[e, (zi + k) % Z].astype(F32)
        fin[e, core, zi] = total.astype(BF)
        for k in range(1, Z):
            gather_copy(e, k).start()
        forward_copy(e, 0).start()

    def returns(e):
        for k in range(1, Z):
            gather_copy(e, k).wait()
            forward_copy(e, k).start()

    def expert(e, carry):
        layer_one = w1_ref[e]
        layer_two = w2_ref[e]
        layer_three = w3p[e]
        lat_part = jnp.concatenate([layer_one[:LAT]] * LO, axis=0)
        wide_one = jnp.concatenate([lat_part, layer_one[LAT:]], axis=0)

        def chunk(b, carry):
            width = SB * CAP
            v = jnp.concatenate(
                [
                    slot_recv[b * SB + i, pl.ds(pl.multiple_of(e * VROWS, VROWS), VROWS), :]
                    for i in range(SB)
                ],
                axis=1,
            ).astype(F32)
            target = v[:OUTC] + v[OUTC : 2 * OUTC]
            hi = v[2 * OUTC : 2 * OUTC + 1]
            tlo = v[2 * OUTC + 1 : 2 * OUTC + 2]
            di = v[2 * OUTC + 2 : 2 * OUTC + 3].astype(jnp.int32)
            hi = hi.astype(jnp.int32)
            tlo = tlo.astype(jnp.int32)
            tile = tlo // LO
            low = tlo % LO
            count = lax.broadcasted_iota(jnp.int32, (HI, width), 0) + 1
            hots = [hot(count == jnp.where(tile == t, hi, 0)) for t in range(T)]
            hots = jnp.concatenate(hots, axis=0)
            spot = jnp.broadcast_to(low, (LAT, width))

            def in_place(wide):
                return jnp.concatenate(
                    [
                        jnp.where(spot == l, wide[l * LAT : (l + 1) * LAT], 0.0).astype(BF)
                        for l in range(LO)
                    ],
                    axis=0,
                )

            found = in_place(nn(texture[...], hots))
            dir_hot = hot(lax.broadcasted_iota(jnp.int32, (NDIR, width), 0) + 1 == di)
            dir_part = nn(dirt_ref[...], dir_hot).astype(BF)
            x = jnp.concatenate([found, dir_part], axis=0)
            pre_one = tn(wide_one, x)
            sig_one = 0.5 * jnp.tanh(0.5 * pre_one) + 0.5
            silu_one = pre_one * sig_one
            act_one = silu_one.astype(BF)
            slope_one = sig_one + silu_one * (1.0 - sig_one)
            pre_two = tn(layer_two, act_one)
            sig_two = 0.5 * jnp.tanh(0.5 * pre_two) + 0.5
            silu_two = pre_two * sig_two
            act_two = silu_two.astype(BF)
            slope_two = sig_two + silu_two * (1.0 - sig_two)
            predicted = nn(layer_three, act_two)
            for i in range(SB):
                ps_send[b * SB + i, e] = predicted[:8, i * CAP : (i + 1) * CAP]
            misfit = (
                predicted
                - jnp.concatenate([target, jnp.zeros((VROWS - OUTC, width), F32)], axis=0)
            ).astype(BF)
            grad_three = nt(misfit, act_two)
            delta_two = (tn(layer_three, misfit) * slope_two).astype(BF)
            grad_two = nt(act_one, delta_two)
            delta_one = (nn(layer_two, delta_two) * slope_one).astype(BF)
            grad_one = nt(x, delta_one)
            dg_acc[...] += nt(in_place(nn(lat_part, delta_one)), hots)
            two, three = slice(LAT + DIRF, first), slice(first, first + VROWS)
            if N == SB:
                g1_acc[...] = grad_one
                gfull[e, two] = grad_two
                gfull[e, three] = grad_three
            else:
                g1_acc[...] += grad_one
                gfull[e, two] += grad_two
                gfull[e, three] += grad_three
            return carry

        gfull[e, first:] = jnp.zeros((CH - first, HID), F32)
        if N == SB:
            chunk(0, 0)
        else:
            g1_acc[...] = jnp.zeros(g1_acc.shape, F32)
            gfull[e, :first] = jnp.zeros((first, HID), F32)
            lax.fori_loop(0, N // SB, chunk, 0)
        lat_grad = g1_acc[0:LAT]
        for l in range(1, LO):
            lat_grad = lat_grad + g1_acc[l * LAT : (l + 1) * LAT]
        gfull[e, 0:LAT] = lat_grad
        gfull[e, LAT : LAT + DIRF] = g1_acc[K:]
        for z in range(Z):
            their = (1 - core) * (CH // 2) + z * RC
            hs_send[e, z] = gfull[e, pl.ds(pl.multiple_of(their, 8), RC), :].astype(BF)
        half_copy(e).start()
        pl.when(e >= 1)(lambda: halves(e - 1))
        pl.when(e >= 2)(lambda: parts(e - 2))
        pl.when(e >= 3)(lambda: returns(e - 3))
        return carry

    lax.fori_loop(0, L, expert, 0)

    def pred_copy(k):
        peer = (me + k) % N
        return remote(ps_send.at[peer], ps_recv.at[me], ps_sems, (k - 1,), {"exp": peer})

    def dense_copy(k):
        peer = (me + k) % N
        return remote(dg_send.at[peer], dg_recv.at[me], dg_sems, (k - 1,), {"exp": peer})

    for k in range(1, N):
        pred_copy(k).start()
    ps_recv[me] = ps_send[me]
    for d in range(N):
        for t in range(T):
            dg_send[d, t] = dg_acc[
                d * PL : (d + 1) * PL, t * HI : (t + 1) * HI
            ].astype(BF)
    for k in range(1, N):
        dense_copy(k).start()

    def save_one(e):
        return pltpu.make_async_copy(
            gfull.at[e, 0 : LAT + DIRF], hbm_out[4].at[e], grad_sems.at[0, e]
        )

    def save_two(e):
        return pltpu.make_async_copy(
            gfull.at[e, LAT + DIRF : first], hbm_out[5].at[e], grad_sems.at[1, e]
        )

    def finish(e):
        for k in range(Z):
            forward_copy(e, k).wait()
        for h in range(2):
            for z in range(Z):
                start = (h * Z + z) * RC
                gfull[e, start : start + RC] = fin[e, h, z].astype(F32)
        save_one(e).start()
        save_two(e).start()

    halves(L - 1)
    if L > 1:
        parts(L - 2)
    if L > 2:
        returns(L - 3)
    for e in range(L - 3):
        finish(e)

    for k in range(1, N):
        dense_copy(k).wait()
    for t in range(T):
        grad = dg_acc[
            pl.ds(pl.multiple_of(me * PL, 8), PL), t * HI : (t + 1) * HI
        ]
        for k in range(1, N):
            grad = grad + dg_recv[(me + k) % N, t].astype(F32)
        for l in range(LOL):
            lanes = slice(l * HI, (l + 1) * HI)
            g = grad[l * LAT : (l + 1) * LAT]
            new_mean = decay_one * mean_ref[t, :, lanes] + (1.0 - decay_one) * g
            new_sq = decay_two * sq_ref[t, :, lanes] + (1.0 - decay_two) * g * g
            nmean_ref[t, :, lanes] = new_mean
            nsq_ref[t, :, lanes] = new_sq
            nlat_ref[t, :, lanes] = lat_ref[t, :, lanes] - step_rate * new_mean / (
                jnp.sqrt(new_sq) + epsilon
            )

    for i in range(3):
        save(i).start()
    parts(L - 1)
    if L > 1:
        returns(L - 2)
    if L > 2:
        finish(L - 3)

    for k in range(1, N):
        pred_copy(k).wait()
    slots = ps_recv[...].reshape(E * 8, CAP)
    slots_hi = slots.astype(BF)
    slots_lo = (slots - slots_hi.astype(F32)).astype(BF)
    back = nn(slots_hi, q_ref[...]) + nn(slots_lo, q_ref[...])
    mat = mat_ref[...]
    mine = jnp.zeros((8, S), F32)
    for e in range(E):
        mine = mine + jnp.where(mat == e, back[e * 8 : (e + 1) * 8], 0.0)
    pred_ref[...] = mine[:OUTC]

    save(3).start()
    if L > 1:
        finish(L - 2)
    returns(L - 1)
    finish(L - 1)
    for e in range(L):
        for c in range(OUTC):
            g3_ref[c, e : e + 1] = gfull[e, first + c : first + c + 1]
    save(6).start()
    for i in (0, 1, 2, 3, 6):
        save(i).wait()
    for e in range(L):
        save_one(e).wait()
        save_two(e).wait()


def on_device(N, R, *args):
    latents, _, _, weight_one, weight_two, weight_three, dir_table = args[:7]
    materials, tile_ids, texel_ids, dir_ids, targets = args[7:]
    T, LAT, texl = latents.shape
    L, width, HID = weight_one.shape
    OUTC = weight_three.shape[1]
    weight_three = weight_three.transpose(1, 0, 2)
    DIRF = dir_table.shape[1]
    S = materials.shape[0]
    E = L * N
    CAP = max(128, 2 * S // E)
    HI = min(256, texl)
    LOL = texl // HI
    LO = N * LOL
    Z = R // 2
    unit = 8 * R
    CH = -(-(width + HID + VROWS) // unit) * unit
    RC = CH // R
    K = LO * LAT
    cfg = dict(
        N=N, R=R, E=E, L=L, S=S, CAP=CAP, HI=HI, LOL=LOL, LO=LO, LAT=LAT, DIRF=DIRF,
        HID=HID, T=T, Z=Z, OUTC=OUTC, CH=CH, RC=RC, SB=min(4, N),
    )
    flat = [a.reshape(1, S) for a in (materials, tile_ids, texel_ids, dir_ids)]
    hbm = pl.BlockSpec(memory_space=pltpu.HBM)
    operands = (*args[:5], weight_three, dir_table.T, *flat, targets)
    operands = tuple(pltpu.with_memory_space_constraint(a, pltpu.HBM) for a in operands)
    outs = (
        jax.ShapeDtypeStruct(latents.shape, F32),
        jax.ShapeDtypeStruct(latents.shape, F32),
        jax.ShapeDtypeStruct(latents.shape, F32),
        jax.ShapeDtypeStruct(targets.shape, F32),
        jax.ShapeDtypeStruct(weight_one.shape, F32),
        jax.ShapeDtypeStruct(weight_two.shape, F32),
        jax.ShapeDtypeStruct(weight_three.shape, F32),
    )
    dma = pltpu.SemaphoreType.DMA
    scratch = [pltpu.VMEM(a.shape, a.dtype) for a in (*operands, *outs[:4], outs[6])]
    scratch += [
        pltpu.VMEM((N, T, LOL * LAT, HI), BF),
        pltpu.VMEM((N, L * VROWS, CAP), BF),
        pltpu.VMEM((N, L * VROWS, CAP), BF),
        pltpu.VMEM((CAP, S), BF),
        pltpu.VMEM((N, L, 8, CAP), F32),
        pltpu.VMEM((N, L, 8, CAP), F32),
        pltpu.VMEM((K, T * HI), F32),
        pltpu.VMEM((N, T, LOL * LAT, HI), BF),
        pltpu.VMEM((N, T, LOL * LAT, HI), BF),
        pltpu.VMEM((K + DIRF, HID), F32),
        pltpu.VMEM((L, CH, HID), F32),
        pltpu.VMEM((L, Z, RC, HID), BF),
        pltpu.VMEM((L, Z, RC, HID), BF),
        pltpu.VMEM((L, Z, RC, HID), BF),
        pltpu.VMEM((L, Z, RC, HID), BF),
        pltpu.VMEM((L, 2, Z, RC, HID), BF),
        pltpu.VMEM((L, VROWS, HID), BF),
        pltpu.VMEM((K, T * HI), BF),
        dma((2, N - 1)),
        dma((2, N - 1)),
        dma((2, N - 1)),
        dma((2, N - 1)),
        dma((2, L)),
        dma((2, L, Z - 1)),
        dma((2, L, Z - 1)),
        dma((2, L, Z)),
        dma((12,)),
        dma((7,)),
        dma((2, L)),
    ]
    results = pl.pallas_call(
        functools.partial(step_kernel, cfg),
        out_shape=tuple(pltpu.HBM(a.shape, a.dtype) for a in outs),
        in_specs=[hbm] * 12,
        out_specs=tuple([hbm] * 7),
        scratch_shapes=scratch,
        compiler_params=pltpu.CompilerParams(
            collective_id=0, has_side_effects=True, vmem_limit_bytes=50 * 2**20
        ),
    )(*operands)
    return (*results[:6], results[6].transpose(1, 0, 2))


def solution(mesh):
    tex = P("rep", None, "exp")
    own = P("exp", None, None)
    rows = P(("rep", "exp"))
    in_specs = (
        tex, tex, tex, own, own, own, P(), P(("rep", "exp"), None), rows, rows, rows,
        P(None, ("rep", "exp")),
    )
    out_specs = (tex, tex, tex, P(None, ("rep", "exp")), own, own, own)
    return jax.shard_map(
        functools.partial(on_device, mesh.shape["exp"], mesh.shape["rep"]),
        mesh=mesh,
        in_specs=in_specs,
        out_specs=out_specs,
        check_vma=False,
    )
```

```python
import functools

import jax
import jax.numpy as jnp
from jax import lax
from jax.experimental import pallas as pl
from jax.experimental.pallas import tpu as pltpu
from jax.sharding import PartitionSpec as P

BF = jnp.bfloat16
F32 = jnp.float32
MESH = pl.DeviceIdType.MESH
decay_one = 0.9
decay_two = 0.99
step_rate = 0.05
epsilon = 1e-08
VROWS = 16


def nn(a, b):
    return lax.dot_general(a, b, (((1,), (0,)), ((), ())), preferred_element_type=F32)


def nt(a, b):
    return lax.dot_general(a, b, (((1,), (1,)), ((), ())), preferred_element_type=F32)


def tn(a, b):
    return lax.dot_general(a, b, (((0,), (0,)), ((), ())), preferred_element_type=F32)


def hot(cond):
    return jnp.where(cond, 1.0, 0.0).astype(BF)


def step_kernel(
    cfg,
    *refs,
):
    hbm_in, hbm_out, rest = refs[:12], refs[12:19], refs[19:]
    (
        lat_ref,
        mean_ref,
        sq_ref,
        w1_ref,
        w2_ref,
        w3_ref,
        dirt_ref,
        mat_ref,
        tile_ref,
        texel_ref,
        dir_ref,
        tgt_ref,
    ) = rest[:12]
    (
        nlat_ref,
        nmean_ref,
        nsq_ref,
        pred_ref,
        g3_ref,
    ) = rest[12:17]
    (
        tex,
        slot_send,
        slot_recv,
        q_ref,
        ps_send,
        ps_recv,
        dg_acc,
        dg_send,
        dg_recv,
        g1_acc,
        gfull,
        hs_send,
        hs_recv,
        zs_send,
        zr_recv,
        fin,
        w3p,
        texture,
        tex_sems,
        slot_sems,
        ps_sems,
        dg_sems,
        hs_sems,
        zr_sems,
        ag_sems,
        fw_sems,
        in_sems,
        out_sems,
        grad_sems,
    ) = rest[17:]
    N, R, E, L = cfg["N"], cfg["R"], cfg["E"], cfg["L"]
    S, CAP, HI, LOL, LO = cfg["S"], cfg["CAP"], cfg["HI"], cfg["LOL"], cfg["LO"]
    LAT, DIRF, HID, T, Z = cfg["LAT"], cfg["DIRF"], cfg["HID"], cfg["T"], cfg["Z"]
    OUTC, CH, RC, SB = cfg["OUTC"], cfg["CH"], cfg["RC"], cfg["SB"]
    NDIR = dirt_ref.shape[1]
    PL = LOL * LAT
    K = LO * LAT
    first = LAT + DIRF + HID
    me = lax.axis_index("exp")
    rep = lax.axis_index("rep")
    core = rep % 2
    zi = rep // 2
    mate = zi * 2 + (1 - core)

    def remote(src, dst, sems, index, peer):
        return pltpu.make_async_remote_copy(
            src_ref=src,
            dst_ref=dst,
            send_sem=sems.at[(0,) + index],
            recv_sem=sems.at[(1,) + index],
            device_id=peer,
            device_id_type=MESH,
        )

    def load(i):
        return pltpu.make_async_copy(hbm_in[i], rest[i], in_sems.at[i])

    def save(i):
        return pltpu.make_async_copy(rest[12 + min(i, 4)], hbm_out[i], out_sems.at[i])

    barrier = pltpu.get_barrier_semaphore()
    for k in range(1, N):
        pl.semaphore_signal(
            barrier, inc=1, device_id={"exp": (me + k) % N}, device_id_type=MESH
        )
    pl.semaphore_signal(barrier, inc=1, device_id={"rep": mate}, device_id_type=MESH)
    for k in range(1, Z):
        pl.semaphore_signal(
            barrier,
            inc=1,
            device_id={"rep": ((zi + k) % Z) * 2 + core},
            device_id_type=MESH,
        )
    for i in (0, 7, 8, 9, 10, 11, 6, 3, 4, 5, 1, 2):
        load(i).start()
    load(0).wait()
    for t in range(T):
        for l in range(LOL):
            tex[me, t, l * LAT : (l + 1) * LAT, :] = lat_ref[
                t, :, l * HI : (l + 1) * HI
            ].astype(BF)
    def tex_copy(k):
        return remote(tex.at[me], tex.at[me], tex_sems, (k - 1,), {"exp": (me + k) % N})

    pl.semaphore_wait(barrier, (N - 1) + 1 + (Z - 1))
    for k in range(1, N):
        tex_copy(k).start()

    for i in range(7, 12):
        load(i).wait()
    mat = mat_ref[...]
    one_hot = jnp.where(
        lax.broadcasted_iota(jnp.int32, (E, S), 0) == mat, 1.0, 0.0
    )
    W = min(256, S)
    blocks = [one_hot[:, b * W : (b + 1) * W] for b in range(S // W)]
    upper = hot(
        lax.broadcasted_iota(jnp.int32, (W, W), 0)
        <= lax.broadcasted_iota(jnp.int32, (W, W), 1)
    )
    cum = nn(jnp.concatenate(blocks, axis=0).astype(BF), upper)
    before = jnp.zeros((E, 1), F32)
    places = []
    for b in range(S // W):
        part = cum[b * E : (b + 1) * E]
        places.append(
            jnp.sum(blocks[b] * (part + (before - 1.0)), axis=0, keepdims=True)
        )
        before = before + part[:, W - 1 : W]
    position = jnp.concatenate(places, axis=1).astype(jnp.int32)
    q = hot(lax.broadcasted_iota(jnp.int32, (CAP, S), 0) == position)
    q_ref[...] = q
    tgt = tgt_ref[...]
    tgt_hi = tgt.astype(BF).astype(F32)
    tgt_lo = tgt - tgt_hi
    texel = texel_ref[...]
    values = jnp.concatenate(
        [
            tgt_hi,
            tgt_lo,
            (texel % HI + 1).astype(F32),
            (tile_ref[...] * LO + texel // HI).astype(F32),
            (dir_ref[...] + 1).astype(F32),
            jnp.zeros((VROWS - 2 * OUTC - 3, S), F32),
        ],
        axis=0,
    )
    spread = jnp.concatenate(
        [jnp.where(mat == e, values, 0.0).astype(BF) for e in range(E)], axis=0
    )
    routed = nt(spread, q).astype(BF)
    for d in range(N):
        slot_send[d] = routed[d * L * VROWS : (d + 1) * L * VROWS]

    def slot_copy(k):
        peer = (me + k) % N
        return remote(
            slot_send.at[peer], slot_recv.at[me], slot_sems, (k - 1,), {"exp": peer}
        )

    for k in range(1, N):
        slot_copy(k).start()
    slot_recv[me] = slot_send[me]
    dg_acc[...] = jnp.zeros(dg_acc.shape, F32)
    for i in range(1, 7):
        load(i).wait()
    colour = w3_ref[...].astype(F32)
    for e in range(L):
        w3p[e] = jnp.concatenate(
            [colour[c, e : e + 1] for c in range(OUTC)]
            + [jnp.zeros((VROWS - OUTC, HID), F32)],
            axis=0,
        ).astype(BF)
    for k in range(1, N):
        tex_copy(k).wait()
    for t in range(T):
        for d in range(N):
            texture[d * PL : (d + 1) * PL, t * HI : (t + 1) * HI] = tex[d, t]
    for k in range(1, N):
        slot_copy(k).wait()

    def half_copy(e):
        return remote(hs_send.at[e], hs_recv.at[e], hs_sems, (e,), {"rep": mate})

    def z_copy(e, k):
        there = (zi + k) % Z
        return remote(
            zs_send.at[e, there],
            zr_recv.at[e, zi],
            zr_sems,
            (e, k - 1),
            {"rep": there * 2 + core},
        )

    def gather_copy(e, k):
        there = (zi + k) % Z
        piece = fin.at[e, core, zi]
        return remote(piece, piece, ag_sems, (e, k - 1), {"rep": there * 2 + core})

    def forward_copy(e, k):
        piece = fin.at[e, core, (zi + Z - k) % Z]
        return remote(piece, piece, fw_sems, (e, k), {"rep": mate})

    def halves(e):
        half_copy(e).wait()
        for z in range(Z):
            own = gfull[e, pl.ds(pl.multiple_of(core * (CH // 2) + z * RC, 8), RC), :]
            zs_send[e, z] = (own + hs_recv[e, z].astype(F32)).astype(BF)
        for k in range(1, Z):
            z_copy(e, k).start()

    def parts(e):
        for k in range(1, Z):
            z_copy(e, k).wait()
        total = zs_send[e, zi].astype(F32)
        for k in range(1, Z):
            total = total + zr_recv[e, (zi + k) % Z].astype(F32)
        fin[e, core, zi] = total.astype(BF)
        for k in range(1, Z):
            gather_copy(e, k).start()
        forward_copy(e, 0).start()

    def returns(e):
        for k in range(1, Z):
            gather_copy(e, k).wait()
            forward_copy(e, k).start()

    def expert(e, carry):
        layer_one = w1_ref[e]
        layer_two = w2_ref[e]
        layer_three = w3p[e]
        lat_part = jnp.concatenate([layer_one[:LAT]] * LO, axis=0)
        wide_one = jnp.concatenate([lat_part, layer_one[LAT:]], axis=0)

        def chunk(b, carry):
            width = SB * CAP
            v = jnp.concatenate(
                [
                    slot_recv[b * SB + i, pl.ds(pl.multiple_of(e * VROWS, VROWS), VROWS), :]
                    for i in range(SB)
                ],
                axis=1,
            ).astype(F32)
            target = v[:OUTC] + v[OUTC : 2 * OUTC]
            hi = v[2 * OUTC : 2 * OUTC + 1]
            tlo = v[2 * OUTC + 1 : 2 * OUTC + 2]
            di = v[2 * OUTC + 2 : 2 * OUTC + 3].astype(jnp.int32)
            hi = hi.astype(jnp.int32)
            tlo = tlo.astype(jnp.int32)
            tile = tlo // LO
            low = tlo % LO
            count = lax.broadcasted_iota(jnp.int32, (HI, width), 0) + 1
            hots = [hot(count == jnp.where(tile == t, hi, 0)) for t in range(T)]
            hots = jnp.concatenate(hots, axis=0)
            spot = jnp.broadcast_to(low, (LAT, width))

            def in_place(wide):
                return jnp.concatenate(
                    [
                        jnp.where(spot == l, wide[l * LAT : (l + 1) * LAT], 0.0).astype(BF)
                        for l in range(LO)
                    ],
                    axis=0,
                )

            found = in_place(nn(texture[...], hots))
            dir_hot = hot(lax.broadcasted_iota(jnp.int32, (NDIR, width), 0) + 1 == di)
            dir_part = nn(dirt_ref[...], dir_hot).astype(BF)
            x = jnp.concatenate([found, dir_part], axis=0)
            pre_one = tn(wide_one, x)
            sig_one = 0.5 * jnp.tanh(0.5 * pre_one) + 0.5
            silu_one = pre_one * sig_one
            act_one = silu_one.astype(BF)
            slope_one = sig_one + silu_one * (1.0 - sig_one)
            pre_two = tn(layer_two, act_one)
            sig_two = 0.5 * jnp.tanh(0.5 * pre_two) + 0.5
            silu_two = pre_two * sig_two
            act_two = silu_two.astype(BF)
            slope_two = sig_two + silu_two * (1.0 - sig_two)
            predicted = nn(layer_three, act_two)
            for i in range(SB):
                ps_send[b * SB + i, e] = predicted[:8, i * CAP : (i + 1) * CAP]
            misfit = (
                predicted
                - jnp.concatenate([target, jnp.zeros((VROWS - OUTC, width), F32)], axis=0)
            ).astype(BF)
            grad_three = nt(misfit, act_two)
            delta_two = (tn(layer_three, misfit) * slope_two).astype(BF)
            grad_two = nt(act_one, delta_two)
            delta_one = (nn(layer_two, delta_two) * slope_one).astype(BF)
            grad_one = nt(x, delta_one)
            dg_acc[...] += nt(in_place(nn(lat_part, delta_one)), hots)
            two, three = slice(LAT + DIRF, first), slice(first, first + VROWS)
            if N == SB:
                g1_acc[...] = grad_one
                gfull[e, two] = grad_two
                gfull[e, three] = grad_three
            else:
                g1_acc[...] += grad_one
                gfull[e, two] += grad_two
                gfull[e, three] += grad_three
            return carry

        gfull[e, first:] = jnp.zeros((CH - first, HID), F32)
        if N == SB:
            chunk(0, 0)
        else:
            g1_acc[...] = jnp.zeros(g1_acc.shape, F32)
            gfull[e, :first] = jnp.zeros((first, HID), F32)
            lax.fori_loop(0, N // SB, chunk, 0)
        lat_grad = g1_acc[0:LAT]
        for l in range(1, LO):
            lat_grad = lat_grad + g1_acc[l * LAT : (l + 1) * LAT]
        gfull[e, 0:LAT] = lat_grad
        gfull[e, LAT : LAT + DIRF] = g1_acc[K:]
        for z in range(Z):
            their = (1 - core) * (CH // 2) + z * RC
            hs_send[e, z] = gfull[e, pl.ds(pl.multiple_of(their, 8), RC), :].astype(BF)
        half_copy(e).start()
        pl.when(e >= 1)(lambda: halves(e - 1))
        pl.when(e >= 2)(lambda: parts(e - 2))
        pl.when(e >= 3)(lambda: returns(e - 3))
        return carry

    lax.fori_loop(0, L, expert, 0)

    def pred_copy(k):
        peer = (me + k) % N
        return remote(ps_send.at[peer], ps_recv.at[me], ps_sems, (k - 1,), {"exp": peer})

    def dense_copy(k):
        peer = (me + k) % N
        return remote(dg_send.at[peer], dg_recv.at[me], dg_sems, (k - 1,), {"exp": peer})

    def save_one(e):
        return pltpu.make_async_copy(
            gfull.at[e, 0 : LAT + DIRF], hbm_out[4].at[e], grad_sems.at[0, e]
        )

    def save_two(e):
        return pltpu.make_async_copy(
            gfull.at[e, LAT + DIRF : first], hbm_out[5].at[e], grad_sems.at[1, e]
        )

    def finish(e):
        for k in range(Z):
            forward_copy(e, k).wait()
        for h in range(2):
            for z in range(Z):
                start = (h * Z + z) * RC
                gfull[e, start : start + RC] = fin[e, h, z].astype(F32)
        save_one(e).start()
        save_two(e).start()

    for d in range(N):
        for t in range(T):
            dg_send[d, t] = dg_acc[
                d * PL : (d + 1) * PL, t * HI : (t + 1) * HI
            ].astype(BF)
    for k in range(1, N):
        dense_copy(k).start()
    for k in range(1, N):
        pred_copy(k).start()
    ps_recv[me] = ps_send[me]
    halves(L - 1)
    if L > 1:
        parts(L - 2)
    if L > 2:
        returns(L - 3)
    for e in range(L - 3):
        finish(e)

    for k in range(1, N):
        dense_copy(k).wait()
    for t in range(T):
        grad = dg_acc[
            pl.ds(pl.multiple_of(me * PL, 8), PL), t * HI : (t + 1) * HI
        ]
        for k in range(1, N):
            grad = grad + dg_recv[(me + k) % N, t].astype(F32)
        for l in range(LOL):
            lanes = slice(l * HI, (l + 1) * HI)
            g = grad[l * LAT : (l + 1) * LAT]
            new_mean = decay_one * mean_ref[t, :, lanes] + (1.0 - decay_one) * g
            new_sq = decay_two * sq_ref[t, :, lanes] + (1.0 - decay_two) * g * g
            nmean_ref[t, :, lanes] = new_mean
            nsq_ref[t, :, lanes] = new_sq
            nlat_ref[t, :, lanes] = lat_ref[t, :, lanes] - step_rate * new_mean / (
                jnp.sqrt(new_sq) + epsilon
            )

    for i in range(3):
        save(i).start()
    parts(L - 1)
    if L > 1:
        returns(L - 2)
    if L > 2:
        finish(L - 3)

    if L > 1:
        finish(L - 2)
    returns(L - 1)
    for k in range(1, N):
        pred_copy(k).wait()
    slots = ps_recv[...].reshape(E * 8, CAP)
    slots_hi = slots.astype(BF)
    slots_lo = (slots - slots_hi.astype(F32)).astype(BF)
    back = nn(slots_hi, q_ref[...]) + nn(slots_lo, q_ref[...])
    mat = mat_ref[...]
    mine = jnp.zeros((8, S), F32)
    for e in range(E):
        mine = mine + jnp.where(mat == e, back[e * 8 : (e + 1) * 8], 0.0)
    pred_ref[...] = mine[:OUTC]

    save(3).start()
    finish(L - 1)
    for e in range(L):
        for c in range(OUTC):
            g3_ref[c, e : e + 1] = gfull[e, first + c : first + c + 1]
    save(6).start()
    for i in (0, 1, 2, 3, 6):
        save(i).wait()
    for e in range(L):
        save_one(e).wait()
        save_two(e).wait()


def on_device(N, R, *args):
    latents, _, _, weight_one, weight_two, weight_three, dir_table = args[:7]
    materials, tile_ids, texel_ids, dir_ids, targets = args[7:]
    T, LAT, texl = latents.shape
    L, width, HID = weight_one.shape
    OUTC = weight_three.shape[1]
    weight_three = weight_three.transpose(1, 0, 2)
    DIRF = dir_table.shape[1]
    S = materials.shape[0]
    E = L * N
    CAP = max(128, 2 * S // E)
    HI = min(256, texl)
    LOL = texl // HI
    LO = N * LOL
    Z = R // 2
    unit = 8 * R
    CH = -(-(width + HID + VROWS) // unit) * unit
    RC = CH // R
    K = LO * LAT
    cfg = dict(
        N=N, R=R, E=E, L=L, S=S, CAP=CAP, HI=HI, LOL=LOL, LO=LO, LAT=LAT, DIRF=DIRF,
        HID=HID, T=T, Z=Z, OUTC=OUTC, CH=CH, RC=RC, SB=min(4, N),
    )
    flat = [a.reshape(1, S) for a in (materials, tile_ids, texel_ids, dir_ids)]
    hbm = pl.BlockSpec(memory_space=pltpu.HBM)
    operands = (*args[:5], weight_three, dir_table.T, *flat, targets)
    operands = tuple(pltpu.with_memory_space_constraint(a, pltpu.HBM) for a in operands)
    outs = (
        jax.ShapeDtypeStruct(latents.shape, F32),
        jax.ShapeDtypeStruct(latents.shape, F32),
        jax.ShapeDtypeStruct(latents.shape, F32),
        jax.ShapeDtypeStruct(targets.shape, F32),
        jax.ShapeDtypeStruct(weight_one.shape, F32),
        jax.ShapeDtypeStruct(weight_two.shape, F32),
        jax.ShapeDtypeStruct(weight_three.shape, F32),
    )
    dma = pltpu.SemaphoreType.DMA
    scratch = [pltpu.VMEM(a.shape, a.dtype) for a in (*operands, *outs[:4], outs[6])]
    scratch += [
        pltpu.VMEM((N, T, LOL * LAT, HI), BF),
        pltpu.VMEM((N, L * VROWS, CAP), BF),
        pltpu.VMEM((N, L * VROWS, CAP), BF),
        pltpu.VMEM((CAP, S), BF),
        pltpu.VMEM((N, L, 8, CAP), F32),
        pltpu.VMEM((N, L, 8, CAP), F32),
        pltpu.VMEM((K, T * HI), F32),
        pltpu.VMEM((N, T, LOL * LAT, HI), BF),
        pltpu.VMEM((N, T, LOL * LAT, HI), BF),
        pltpu.VMEM((K + DIRF, HID), F32),
        pltpu.VMEM((L, CH, HID), F32),
        pltpu.VMEM((L, Z, RC, HID), BF),
        pltpu.VMEM((L, Z, RC, HID), BF),
        pltpu.VMEM((L, Z, RC, HID), BF),
        pltpu.VMEM((L, Z, RC, HID), BF),
        pltpu.VMEM((L, 2, Z, RC, HID), BF),
        pltpu.VMEM((L, VROWS, HID), BF),
        pltpu.VMEM((K, T * HI), BF),
        dma((2, N - 1)),
        dma((2, N - 1)),
        dma((2, N - 1)),
        dma((2, N - 1)),
        dma((2, L)),
        dma((2, L, Z - 1)),
        dma((2, L, Z - 1)),
        dma((2, L, Z)),
        dma((12,)),
        dma((7,)),
        dma((2, L)),
    ]
    results = pl.pallas_call(
        functools.partial(step_kernel, cfg),
        out_shape=outs,
        in_specs=[hbm] * 12,
        out_specs=tuple([hbm] * 7),
        scratch_shapes=scratch,
        compiler_params=pltpu.CompilerParams(
            collective_id=0, has_side_effects=True, vmem_limit_bytes=50 * 2**20
        ),
    )(*operands)
    return (*results[:6], results[6].transpose(1, 0, 2))


def solution(mesh):
    tex = P("rep", None, "exp")
    own = P("exp", None, None)
    rows = P(("rep", "exp"))
    in_specs = (
        tex, tex, tex, own, own, own, P(), P(("rep", "exp"), None), rows, rows, rows,
        P(None, ("rep", "exp")),
    )
    out_specs = (tex, tex, tex, P(None, ("rep", "exp")), own, own, own)
    return jax.shard_map(
        functools.partial(on_device, mesh.shape["exp"], mesh.shape["rep"]),
        mesh=mesh,
        in_specs=in_specs,
        out_specs=out_specs,
        check_vma=False,
    )
```
